8 devices in a mesh: dp: 2 (over z, y), cp: 4 (over x, core).
Axes of the slice: x: 2, y: 2, z: 1, core: 2. Of those that a mesh axis runs over, the one named last changes fastest.
Arguments:
- x_act: bfloat16 [4, 2048, 2048], P('dp', 'cp')
- d_out: bfloat16 [4, 2048, 2048], P('dp', 'cp')
- seg_ids: int32 [4, 2048], P('dp', 'cp')
- w_q: bfloat16 [2048, 16, 128], replicated
- w_k: bfloat16 [2048, 16, 128], replicated
- w_v: bfloat16 [2048, 16, 128], replicated
- w_o: bfloat16 [16, 128, 2048], replicated
- w_up: bfloat16 [2048, 8192], replicated
- w_down: bfloat16 [8192, 2048], replicated
Outputs:
- output 1: bfloat16 [4, 2048, 2048], P('dp', 'cp')
- output 2: float32 [2048, 16, 128], replicated
- output 3: float32 [2048, 16, 128], replicated
- output 4: float32 [2048, 16, 128], replicated
- output 5: float32 [16, 128, 2048], replicated
- output 6: float32 [2048, 8192], replicated
- output 7: float32 [8192, 2048], replicated
All inputs are finite; a program needn't handle non-finite values.
Results may differ from the reference program's by a relative error of at most 0.017864.
Values are sent between devices in bfloat16 or wider.
A program may use at most 1.25 GiB of HBM per device.

```python
import jax
import jax.numpy as jnp
from jax import lax

MODEL_DIM = 2048
HEADS = 16
KV_HEADS = 16
HEAD_DIM = 128
FFN_DIM = 8192
BATCH = 4
SEQ_LEN = 2048
CP_SIZE = 4
WORKERS = 8
NUM_DOCS = 4

GROUP_SIZE = HEADS // KV_HEADS
PIECE_LEN = SEQ_LEN // (2 * CP_SIZE)
SCORE_SCALE = HEAD_DIM ** -0.5


def bf16_value(val_in):
    return val_in + lax.stop_gradient(val_in.astype(jnp.bfloat16).astype(jnp.float32) - val_in)


def to_true_order(array_in):
    shaped = array_in.reshape((array_in.shape[0], CP_SIZE, 2, PIECE_LEN) + array_in.shape[2:])
    front_part = shaped[:, :, 0]
    back_part = jnp.flip(shaped[:, :, 1], axis=1)
    return jnp.concatenate([front_part, back_part], axis=1).reshape(array_in.shape)


def to_stored_order(array_in):
    shaped = array_in.reshape((array_in.shape[0], 2, CP_SIZE, PIECE_LEN) + array_in.shape[2:])
    front_part = shaped[:, 0]
    back_part = jnp.flip(shaped[:, 1], axis=1)
    return jnp.stack([front_part, back_part], axis=2).reshape(array_in.shape)


def draw_weight(rng_key, arr_shape, std_dev):
    return (jax.random.normal(rng_key, arr_shape, jnp.float32) * std_dev).astype(jnp.bfloat16)


def setup_inputs(seed: int = 0) -> dict:
    keys = jax.random.split(jax.random.key(seed), 9)
    attn_gain = (SEQ_LEN / (8.0 * NUM_DOCS)) ** 0.5
    qk_std = 0.7 * MODEL_DIM ** -0.5
    x_act = jax.random.normal(keys[0], (BATCH, SEQ_LEN, MODEL_DIM), jnp.float32)
    d_out = jax.random.normal(keys[1], (BATCH, SEQ_LEN, MODEL_DIM), jnp.float32)
    cut_points = jnp.sort(jax.random.randint(keys[2], (BATCH, NUM_DOCS - 1), 1, SEQ_LEN), axis=1)
    positions = jnp.arange(SEQ_LEN, dtype=jnp.int32)
    seg_true = jnp.sum((positions[None, :, None] >= cut_points[:, None, :]).astype(jnp.int32), axis=2)
    return {
        'x_act': x_act.astype(jnp.bfloat16),
        'd_out': d_out.astype(jnp.bfloat16),
        'seg_ids': to_stored_order(seg_true).astype(jnp.int32),
        'w_q': draw_weight(keys[3], (MODEL_DIM, HEADS, HEAD_DIM), qk_std),
        'w_k': draw_weight(keys[4], (MODEL_DIM, KV_HEADS, HEAD_DIM), qk_std),
        'w_v': draw_weight(keys[5], (MODEL_DIM, KV_HEADS, HEAD_DIM), MODEL_DIM ** -0.5),
        'w_o': draw_weight(keys[6], (HEADS, HEAD_DIM, MODEL_DIM), attn_gain * (HEADS * HEAD_DIM) ** -0.5),
        'w_up': draw_weight(keys[7], (MODEL_DIM, FFN_DIM), MODEL_DIM ** -0.5),
        'w_down': draw_weight(keys[8], (FFN_DIM, MODEL_DIM), FFN_DIM ** -0.5),
    }


def layer_one(x_seq, seg_seq, q_weight, k_weight, v_weight, o_weight, up_weight, down_weight):
    queries = bf16_value(jnp.einsum('sd,dnk->snk', x_seq, q_weight)).reshape(SEQ_LEN // PIECE_LEN, PIECE_LEN, KV_HEADS, GROUP_SIZE, HEAD_DIM)
    key_act = bf16_value(jnp.einsum('sd,dnk->snk', x_seq, k_weight))
    value_act = bf16_value(jnp.einsum('sd,dnk->snk', x_seq, v_weight))
    positions = jnp.arange(SEQ_LEN)

    def block_attention(block_in):
        q_blk, q_seg, q_pos = block_in
        scores = jnp.einsum('qngk,tnk->ngqt', q_blk, key_act) * SCORE_SCALE
        allowed = (q_pos[:, None] >= positions[None, :]) & (q_seg[:, None] == seg_seq[None, :])
        scores = jnp.where(allowed[None, None], scores, -1e30)
        probs_row = bf16_value(jax.nn.softmax(scores, axis=-1))
        return jnp.einsum('ngqt,tnk->qngk', probs_row, value_act)

    attn_out = lax.map(jax.checkpoint(block_attention), (queries, seg_seq.reshape(-1, PIECE_LEN), positions.reshape(-1, PIECE_LEN)))
    attn_out = bf16_value(attn_out.reshape(SEQ_LEN, HEADS, HEAD_DIM))
    hidden = bf16_value(x_seq + jnp.einsum('snk,nkd->sd', attn_out, o_weight))
    act_out = bf16_value(jax.nn.gelu(jnp.dot(hidden, up_weight), approximate=True))
    return hidden + jnp.dot(act_out, down_weight)


def reference(x_act, d_out, seg_ids, w_q, w_k, w_v, w_o, w_up, w_down):
    weights = tuple(weight.astype(jnp.float32) for weight in (w_q, w_k, w_v, w_o, w_up, w_down))
    x_true = to_true_order(x_act).astype(jnp.float32)
    dout_true = to_true_order(d_out).astype(jnp.float32)
    seg_true = to_true_order(seg_ids)

    def one_sequence(grad_sums, seq_data):
        x_seq, dout_seq, seg_seq = seq_data

        def layer_fn(x_in, q_weight, k_weight, v_weight, o_weight, up_weight, down_weight):
            return layer_one(x_in, seg_seq, q_weight, k_weight, v_weight, o_weight, up_weight, down_weight)

        _, pullback = jax.vjp(layer_fn, x_seq, *weights)
        cotangents = pullback(dout_seq)
        new_sums = tuple(sum_prev + part_grad for sum_prev, part_grad in zip(grad_sums, cotangents[1:]))
        return new_sums, cotangents[0]

    zero_sums = tuple(jnp.zeros_like(weight) for weight in weights)
    grad_sums, dx_true = lax.scan(one_sequence, zero_sums, (x_true, dout_true, seg_true))
    d_x = to_stored_order(dx_true).astype(jnp.bfloat16)
    return (d_x, grad_sums[0] / WORKERS, grad_sums[1] / WORKERS, grad_sums[2] / WORKERS, grad_sums[3] / WORKERS, grad_sums[4] / WORKERS, grad_sums[5] / WORKERS)
```

```python
import functools

import jax
import jax.numpy as jnp
from jax import lax
from jax.experimental import pallas as pl
from jax.experimental.pallas import tpu as pltpu
from jax.sharding import PartitionSpec as P

BF16 = jnp.bfloat16
F32 = jnp.float32
NEG_BIG = -1e30
LOG2E = 1.4426950408889634

CORE_PERM = [(0, 1), (1, 0), (2, 3), (3, 2)]
X_PERM = [(0, 2), (2, 0), (1, 3), (3, 1)]
Y_PERM = [(0, 1), (1, 0)]


def to_core(val):
    return lax.ppermute(val, 'cp', CORE_PERM)


def to_x(val):
    return lax.ppermute(val, 'cp', X_PERM)


def to_y(val):
    return lax.ppermute(val, 'dp', Y_PERM)


def mm(a, b, dims, out=F32):
    return lax.dot_general(a, b, (dims, ((), ())), preferred_element_type=F32).astype(out)


def unit_list(n_src, with_own):
    units = []
    for src in range(n_src):
        own = with_own and src == 0
        for q_piece, k_piece in ((0, 0), (1, 1), (1, 0)):
            diag = own and q_piece == k_piece
            units.append((q_piece, src, k_piece, diag))
    return units


def allowed_mask(segk, segq, diag):
    mask = segk == segq
    if diag:
        rows = lax.broadcasted_iota(jnp.int32, mask.shape, 0)
        cols = lax.broadcasted_iota(jnp.int32, mask.shape, 1)
        mask = mask & (rows <= cols)
    return mask


def attn_fwd_kernel(n_src, first, half, scale2, need_ref, q_ref, segq_ref, *refs):
    k_refs, v_refs, segk_refs = refs[:n_src], refs[n_src:2 * n_src], refs[2 * n_src:3 * n_src]
    rest = refs[3 * n_src:]
    if first:
        acc_out, m_out, l_out = rest
        acc_ref, m_ref, l_ref = acc_out.at[0, 0], m_out.at[0, 0], l_out.at[0, 0]
    else:
        acc_in, m_in, l_in, o_ref, lse_ref, acc_ref, m_ref, l_ref = rest
        acc_ref[...] = acc_in[0, 0]
        m_ref[...] = m_in[0, 0]
        l_ref[...] = l_in[0, 0]
    batch = pl.program_id(0)

    def unit(q_piece, src, k_piece, diag):
        qs = pl.ds(q_piece * half, half)
        ks = pl.ds(k_piece * half, half)
        s_t = mm(k_refs[src][0, ks, :], q_ref[0, qs, :], ((1,), (1,)))
        mask = allowed_mask(segk_refs[src][0, ks, :], segq_ref[0, :, qs], diag)
        t = jnp.where(mask, s_t * scale2, NEG_BIG)
        t_max = jnp.max(t, axis=0, keepdims=True)
        if diag:
            m_new = t_max
        else:
            m_old = m_ref[:, qs]
            m_new = jnp.maximum(m_old, t_max)
        p = jnp.exp2(t - m_new)
        p_sum = jnp.sum(p, axis=0, keepdims=True)
        part = mm(v_refs[src][0, ks, :], p.astype(BF16), ((0,), (0,)))
        m_ref[:, qs] = m_new
        if diag:
            l_ref[:, qs] = p_sum
            acc_ref[:, qs] = part
        else:
            alpha = jnp.exp2(m_old - m_new)
            l_ref[:, qs] = l_ref[:, qs] * alpha + p_sum
            acc_ref[:, qs] = acc_ref[:, qs] * alpha + part

    for q_piece, src, k_piece, diag in unit_list(n_src, first):
        if diag:
            unit(q_piece, src, k_piece, diag)
        else:
            flag = need_ref[((batch * 2 + q_piece) * n_src + src) * 2 + k_piece]
            pl.when(flag > 0)(functools.partial(unit, q_piece, src, k_piece, diag))

    if not first:
        o_t = acc_ref[...] / l_ref[...]
        o_ref[0] = o_t.T.astype(BF16)
        lse_ref[0, 0] = m_ref[...] + jnp.log2(l_ref[...])


def attn_fwd(first, scale2, need, q, segq, ks, vs, segks, state=None):
    n_src = len(ks)
    batch, seq, width = q.shape
    hd = 128
    heads = width // hd
    col = pl.BlockSpec((1, seq, hd), lambda b, h, n: (b, 0, h))
    per_head = lambda rows: pl.BlockSpec((1, 1, rows, seq), lambda b, h, n: (b, h, 0, 0))
    segq_spec = pl.BlockSpec((1, 1, seq), lambda b, h, n: (b, 0, 0))
    segk_spec = pl.BlockSpec((1, seq, seq // 2), lambda b, h, n: (b, 0, 0))
    in_specs = [col, segq_spec] + [col] * (2 * n_src) + [segk_spec] * n_src
    operands = [q, segq, *ks, *vs, *segks]
    shape = lambda rows: jax.ShapeDtypeStruct((batch, heads, rows, seq), F32)
    if first:
        out_shape = (shape(hd), shape(1), shape(1))
        out_specs = (per_head(hd), per_head(1), per_head(1))
        scratch = []
    else:
        in_specs += [per_head(hd), per_head(1), per_head(1)]
        operands += list(state)
        out_shape = (jax.ShapeDtypeStruct(q.shape, BF16), shape(1))
        out_specs = (col, per_head(1))
        scratch = [pltpu.VMEM((hd, seq), F32), pltpu.VMEM((1, seq), F32), pltpu.VMEM((1, seq), F32)]
    pairs = batch * heads * (5 if first else 4) * (seq // 2) ** 2
    return pl.pallas_call(
        functools.partial(attn_fwd_kernel, n_src, first, seq // 2, scale2),
        grid_spec=pltpu.PrefetchScalarGridSpec(
            num_scalar_prefetch=1, grid=(batch, heads), in_specs=in_specs, out_specs=out_specs, scratch_shapes=scratch),
        out_shape=out_shape,
        cost_estimate=pl.CostEstimate(flops=8 * pairs * hd, bytes_accessed=16 << 20, transcendentals=pairs),
        compiler_params=pltpu.CompilerParams(dimension_semantics=("arbitrary", "arbitrary")),
        name="attn_fwd_first" if first else "attn_fwd_last",
    )(need, *operands)


def attn_bwd_kernel(half, scale, need_ref, q_ref, o_ref, do_ref, lse_ref, segq_ref, *refs):
    k_refs, v_refs, segk_refs = refs[0:4], refs[4:8], refs[8:12]
    dq_ref, own_ref, far_ref, send_own_ref, send_far_ref, dk_acc, dv_acc, dq_acc, delta_ref = refs[12:]
    batch = pl.program_id(0)
    seq, hd = 2 * half, 128
    scale2 = scale * LOG2E
    dk_acc[...] = jnp.zeros_like(dk_acc)
    dv_acc[...] = jnp.zeros_like(dv_acc)
    dq_acc[...] = jnp.zeros_like(dq_acc)
    prod = do_ref[0].astype(F32) * o_ref[0].astype(F32)
    delta_ref[...] = lax.dot_general(jnp.ones((8, hd), F32), prod, (((1,), (1,)), ((), ())),
                                     precision=lax.Precision.HIGHEST, preferred_element_type=F32)

    def unit(q_piece, src, k_piece, diag):
        qs = pl.ds(q_piece * half, half)
        ks = pl.ds(k_piece * half, half)
        rows = pl.ds(src * seq + k_piece * half, half)
        k_blk, v_blk = k_refs[src][0, ks, :], v_refs[src][0, ks, :]
        q_blk, do_blk = q_ref[0, qs, :], do_ref[0, qs, :]
        s_t = mm(k_blk, q_blk, ((1,), (1,)))
        dp_t = mm(v_blk, do_blk, ((1,), (1,)))
        mask = allowed_mask(segk_refs[src][0, ks, :], segq_ref[0, :, qs], diag)
        p = jnp.where(mask, jnp.exp2(s_t * scale2 - lse_ref[0, 0, :, qs]), 0.0)
        ds = (p * (dp_t - delta_ref[0:1, qs])).astype(BF16)
        dv_acc[rows, :] += mm(p.astype(BF16), do_blk, ((1,), (0,)))
        dk_acc[rows, :] += mm(ds, q_blk, ((1,), (0,)))
        dq_acc[:, qs] += mm(k_blk, ds, ((0,), (0,)))

    for q_piece, src, k_piece, diag in unit_list(4, True):
        if diag:
            unit(q_piece, src, k_piece, diag)
        else:
            flag = need_ref[((batch * 2 + q_piece) * 4 + src) * 2 + k_piece]
            pl.when(flag > 0)(functools.partial(unit, q_piece, src, k_piece, diag))

    dq_ref[0] = (dq_acc[...] * scale).T.astype(BF16)
    for src, out in ((0, own_ref), (2, far_ref), (1, send_own_ref), (3, send_far_ref)):
        rows = pl.ds(src * seq, seq)
        out[0, 0] = (dk_acc[rows, :] * scale).astype(out.dtype)
        out[1, 0] = dv_acc[rows, :].astype(out.dtype)


def attn_bwd(scale, need, q, o, do, lse, segq, ks, vs, segks):
    batch, seq, width = q.shape
    hd = 128
    heads = width // hd
    col = pl.BlockSpec((1, seq, hd), lambda b, h, n: (b, 0, h))
    segq_spec = pl.BlockSpec((1, 1, seq), lambda b, h, n: (b, 0, 0))
    segk_spec = pl.BlockSpec((1, seq, seq // 2), lambda b, h, n: (b, 0, 0))
    lse_spec = pl.BlockSpec((1, 1, 1, seq), lambda b, h, n: (b, h, 0, 0))
    pair_spec = pl.BlockSpec((2, 1, seq, hd), lambda b, h, n: (0, b, 0, h))
    pair = lambda dt: jax.ShapeDtypeStruct((2,) + q.shape, dt)
    pairs = batch * heads * 9 * (seq // 2) ** 2
    return pl.pallas_call(
        functools.partial(attn_bwd_kernel, seq // 2, scale),
        grid_spec=pltpu.PrefetchScalarGridSpec(
            num_scalar_prefetch=1, grid=(batch, heads),
            in_specs=[col, col, col, lse_spec, segq_spec] + [col] * 8 + [segk_spec] * 4,
            out_specs=(col, pair_spec, pair_spec, pair_spec, pair_spec),
            scratch_shapes=[pltpu.VMEM((4 * seq, hd), F32), pltpu.VMEM((4 * seq, hd), F32),
                            pltpu.VMEM((hd, seq), F32), pltpu.VMEM((8, seq), F32)]),
        out_shape=(jax.ShapeDtypeStruct(q.shape, BF16), pair(F32), pair(F32), pair(BF16), pair(BF16)),
        cost_estimate=pl.CostEstimate(flops=20 * pairs * hd, bytes_accessed=64 << 20, transcendentals=pairs),
        compiler_params=pltpu.CompilerParams(dimension_semantics=("arbitrary", "arbitrary")),
        name="attn_bwd",
    )(need, q, o, do, lse, segq, *ks, *vs, *segks)


def assemble_kernel(three_d, g_ref, *refs):
    out_ref = refs[-1]
    val = g_ref[0].astype(F32)
    if three_d:
        for h in range(16):
            out_ref[:, h, :] = val[:, h * 128:(h + 1) * 128]
    else:
        out_ref[...] = val


def assemble(gathered, prev, row0, total_rows, three_d):
    n_blocks, rows, cols = gathered.shape
    base = row0 // rows

    def src_index(step):
        core, path, i, j = step // 8, (step // 4) % 2, (step // 2) % 2, step % 2
        y_of = path * i + (1 - path) * j
        x_of = path * j + (1 - path) * i
        return ((y_of * 2 + x_of) * 2 + core) * 2 + path

    if three_d:
        out_shape = jax.ShapeDtypeStruct((total_rows, 16, 128), F32)
        out_spec = pl.BlockSpec((rows, 16, 128), lambda s: (base + s, 0, 0))
    else:
        out_shape = jax.ShapeDtypeStruct((total_rows, cols), F32)
        out_spec = pl.BlockSpec((rows, cols), lambda s: (base + s, 0))
    in_specs = [pl.BlockSpec((1, rows, cols), lambda s: (src_index(s), 0, 0))]
    operands = [gathered]
    aliases = {}
    if prev is not None:
        in_specs.append(pl.BlockSpec(memory_space=pl.ANY))
        operands.append(prev)
        aliases = {1: 0}
    return pl.pallas_call(
        functools.partial(assemble_kernel, three_d),
        grid=(n_blocks,), in_specs=in_specs, out_specs=out_spec, out_shape=out_shape,
        input_output_aliases=aliases,
        cost_estimate=pl.CostEstimate(flops=6 * n_blocks * rows * cols, bytes_accessed=6 * n_blocks * rows * cols, transcendentals=0),
        compiler_params=pltpu.CompilerParams(dimension_semantics=("arbitrary",)),
        name="assemble",
    )(*operands)


def solution(mesh):
    cp_size = mesh.shape['cp']
    workers = mesh.shape['dp'] * cp_size

    def local_grads(x_loc, dout_loc, seg_loc, w_q, w_k, w_v, w_o, w_up, w_down):
        batch, seq, dim = x_loc.shape
        tokens = batch * seq
        heads, hd = w_q.shape[1], w_q.shape[2]
        width = heads * hd
        ffn = w_up.shape[1]
        half = seq // 2
        scale = hd ** -0.5
        cp_index = lax.axis_index('cp')
        my_core, my_x, my_y = cp_index % 2, cp_index // 2, lax.axis_index('dp')
        wq2, wk2, wv2 = (w.reshape(dim, width) for w in (w_q, w_k, w_v))
        wo2 = w_o.reshape(width, dim)
        x2 = x_loc.reshape(tokens, dim)
        dout2 = dout_loc.reshape(tokens, dim)
        as_seq = lambda val: val.reshape(batch, seq, val.shape[-1])
        flat = lambda val: val.reshape(tokens, val.shape[-1])

        x_far = to_x(x_loc)
        seg_pair = to_core(seg_loc)
        seg_far = to_x(seg_loc)
        seg_far_pair = to_core(seg_far)
        owners = [cp_index, cp_index ^ 1, cp_index ^ 2, cp_index ^ 3]
        segs = [seg_loc, seg_pair, seg_far, seg_far_pair]
        pieces = [jnp.stack([owner, 2 * cp_size - 1 - owner]) for owner in owners]
        q_first = seg_loc.reshape(batch, 2, half)[:, :, 0]
        need = jnp.stack([
            (pieces[src][None, None, :] <= pieces[0][None, :, None])
            & (segs[src].reshape(batch, 2, half)[:, None, :, -1] >= q_first[:, :, None])
            for src in range(4)], axis=2).astype(jnp.int32)
        segq = seg_loc[:, None, :]
        segks = [jnp.broadcast_to(seg_val[:, :, None], (batch, seq, half)) for seg_val in segs]

        def project(x_val, w_val):
            return as_seq(mm(flat(x_val), w_val, ((1,), (0,)), BF16))

        k_own, v_own = project(x_loc, wk2), project(x_loc, wv2)
        k_pair, v_pair = to_core(k_own), to_core(v_own)
        q_own = project(x_loc, wq2)
        scale2 = scale * LOG2E
        state = attn_fwd(True, scale2, need[:, :, :2].reshape(-1), q_own, segq,
                         (k_own, k_pair), (v_own, v_pair), segks[:2])
        d_act = mm(dout2, w_down, ((1,), (1,)))
        k_far, v_far = project(x_far, wk2), project(x_far, wv2)
        k_far_pair, v_far_pair = to_core(k_far), to_core(v_far)
        attn_out, lse = attn_fwd(False, scale2, need[:, :, 2:].reshape(-1), q_own, segq,
                                 (k_far, k_far_pair), (v_far, v_far_pair), segks[2:], state)
        attn2 = flat(attn_out)
        hidden = (x2 + mm(attn2, wo2, ((1,), (0,)))).astype(BF16)

        def reduce_chunk(a_val, b_val):
            rows, cols = a_val.shape[1], b_val.shape[1]
            pick = lambda val, index, size: lax.dynamic_slice_in_dim(val, index * size, size, 0)
            pick_cols = lambda index: lax.dynamic_slice_in_dim(a_val, index * (rows // 2), rows // 2, 1)
            give = mm(pick_cols(1 - my_core), b_val, ((0,), (0,)), BF16)
            got = to_core(give)
            mine = mm(pick_cols(my_core), b_val, ((0,), (0,))) + got.astype(F32)
            quarter, eighth, last = rows // 4, rows // 8, rows // 16
            path_a, path_b = mine[:quarter], mine[quarter:]
            got_a = to_x(pick(path_a, 1 - my_x, eighth).astype(BF16))
            got_b = to_y(pick(path_b, 1 - my_y, eighth).astype(BF16))
            sum_a = pick(path_a, my_x, eighth) + got_a.astype(F32)
            sum_b = pick(path_b, my_y, eighth) + got_b.astype(F32)
            got_a = to_y(pick(sum_a, 1 - my_y, last).astype(BF16))
            got_b = to_x(pick(sum_b, 1 - my_x, last).astype(BF16))
            end_a = (pick(sum_a, my_y, last) + got_a.astype(F32)) / workers
            end_b = (pick(sum_b, my_x, last) + got_b.astype(F32)) / workers
            ends = jnp.stack([end_a, end_b]).astype(BF16)
            return lax.all_gather(ends, ('dp', 'cp'), axis=0, tiled=True).reshape(16, last, cols)

        n_chunk = 4
        f_len = ffn // n_chunk
        d_ups = []
        dw_down = None
        for idx in range(n_chunk):
            cols = slice(idx * f_len, (idx + 1) * f_len)
            up_pre = mm(hidden, w_up[:, cols], ((1,), (0,)))
            act_f32, pull = jax.vjp(lambda val: jax.nn.gelu(val, approximate=True), up_pre)
            d_ups.append(pull(d_act[:, cols])[0].astype(BF16))
            gathered = reduce_chunk(act_f32.astype(BF16), dout2)
            dw_down = assemble(gathered, dw_down, idx * f_len, ffn, False)
        d_up = jnp.concatenate(d_ups, axis=1)
        d_len = dim // n_chunk
        dw_up = None
        for idx in range(n_chunk):
            gathered = reduce_chunk(hidden[:, idx * d_len:(idx + 1) * d_len], d_up)
            dw_up = assemble(gathered, dw_up, idx * d_len, dim, False)
        d_hidden = dout2.astype(F32) + mm(d_up, w_up, ((1,), (1,)))
        d_hidden_b16 = d_hidden.astype(BF16)
        d_attn = as_seq(mm(d_hidden_b16, wo2, ((1,), (1,)), BF16))
        dw_o = assemble(reduce_chunk(attn2, d_hidden_b16), None, 0, width, False)

        dq, own, far, send_own, send_far = attn_bwd(
            scale, need.reshape(-1), q_own, attn_out, d_attn, lse, segq,
            (k_own, k_pair, k_far, k_far_pair), (v_own, v_pair, v_far, v_far_pair), segks)
        got_far = to_core(send_far)
        got_own = to_core(send_own)
        dk_far, dv_far = (flat((far[i] + got_far[i].astype(F32)).astype(BF16)) for i in range(2))
        dx_far = (mm(dk_far, wk2, ((1,), (1,))) + mm(dv_far, wv2, ((1,), (1,)))).astype(BF16)
        dx_got = to_x(dx_far)
        dk_own, dv_own = (flat((own[i] + got_own[i].astype(F32)).astype(BF16)) for i in range(2))
        dq2 = flat(dq)
        x_both = jnp.concatenate([x2, flat(x_far)], axis=0)
        dw_q = assemble(reduce_chunk(x2, dq2), None, 0, dim, True)
        dw_k = assemble(reduce_chunk(x_both, jnp.concatenate([dk_own, dk_far], axis=0)), None, 0, dim, True)
        dw_v = assemble(reduce_chunk(x_both, jnp.concatenate([dv_own, dv_far], axis=0)), None, 0, dim, True)
        d_x = (d_hidden + mm(dq2, wq2, ((1,), (1,))) + mm(dk_own, wk2, ((1,), (1,)))
               + mm(dv_own, wv2, ((1,), (1,))) + dx_got.astype(F32)).astype(BF16)
        return (as_seq(d_x), dw_q, dw_k, dw_v, dw_o.reshape(w_o.shape), dw_up, dw_down)

    act_spec = P('dp', 'cp', None)
    return jax.shard_map(local_grads, mesh=mesh,
                         in_specs=(act_spec, act_spec, P('dp', 'cp'), P(), P(), P(), P(), P(), P()),
                         out_specs=(act_spec, P(), P(), P(), P(), P(), P()),
                         check_vma=False)
```
